32 devices in a mesh: dp: 8 (over z, y), group: 4 (over x, core).
Axes of the slice: x: 2, y: 2, z: 4, core: 2. Of those that a mesh axis runs over, the one named last changes fastest.
Arguments:
- keys: int32 [16384], P(('dp', 'group')), may hold values from 0 to 1073741823
- cut: int32 [1], replicated, may hold values from 256 to 1023
- owner: int32 [16384, 1], P(('dp', 'group')), may hold values from 0 to 7; in each aligned block of 512 rows (0 to 511, 512 to 1023, ...) at most 128 rows name the same one
- tokens: int32 [16384, 2048], P(('dp', 'group')), may hold values from 0 to 128255
Outputs:
- histogram: int32 [4096], replicated
- packed_rows: int32 [32768, 2048], P(('dp', 'group'))
- packed_weights: float32 [32768], P(('dp', 'group'))
The draws below stay inside these ranges and needn't reach their ends.
Inputs may be any that keep to these rules, and one draw needn't show every extreme that they name: Among the examples of one device, at most 128 have the same owner, and some owner has exactly 128.
All inputs are finite; a program needn't handle non-finite values.
Results may differ from the reference program's by a relative error of at most 0.0003.
Values sent between devices are 32-bit elements; how exact they have to be, the bound alone decides.
A program may use at most 128 MiB of HBM per device.

```python
import math
import jax
import jax.numpy as jnp
import numpy as np

EX_DEV = 512
SEQ = 2048
BINS = 4096
BIN_WIDTH = 262144
VOCAB = 128256
EXAMPLES = 16384
MOST = 128
RECV = 1024
N_DP = 8
N_GROUP = 4


def place_ends(array, rng, smallest, top_value):
    extent = array.shape
    place = [jax.random.randint(jax.random.fold_in(rng, axis), (), 0, extent[axis]) for axis in range(len(extent))]
    array = array.at[tuple(place)].set(smallest)
    longest = extent.index(max(extent))
    place[longest] = (place[longest] + 1) % extent[longest]
    return array.at[tuple(place)].set(top_value)


def ranked_wide(rng, extent, amount, slope):
    weights = [min(1 << octave, amount + 1 - (1 << octave)) * (1 << 20) // math.isqrt((1 << octave) ** slope) + 1 for octave in range((amount + 1).bit_length()) if 1 << octave <= amount]
    scale = 1 + sum(weights) // (1 << 30)
    table = np.cumsum(np.array([max(1, weight // scale) for weight in weights]))
    ticket = jax.random.randint(jax.random.fold_in(rng, 1), extent, 0, int(table[len(weights) - 1]))
    start = jnp.left_shift(1, jnp.searchsorted(jnp.asarray(table, jnp.int32), ticket, side="right").astype(jnp.int32))
    rank = start - 1 + jax.random.randint(jax.random.fold_in(rng, 4), extent, 0, 1 << 30) % jnp.minimum(start, amount + 1 - start)
    return jax.random.permutation(jax.random.fold_in(rng, 2), amount)[rank].astype(jnp.int32)


def deal_out(rng, own, number, rows, number_of, top, limit, slope):
    ranking = jax.random.permutation(rng, number_of)
    packed, common = shares(number_of, rows * top, limit, slope, True), shares(number_of, rows * top, limit, slope, False)
    places = jnp.arange(number_of)

    def named(sizes, rotation):
        used = int((sizes > 0).sum())
        fixed = max(1, used // 4)
        moved = fixed + (places - fixed + rotation * (used - fixed)) % max(1, number_of - fixed)
        return jnp.zeros((number_of,), jnp.int32).at[ranking[jnp.where(places < fixed, places, moved)]].set(jnp.asarray(sizes, jnp.int32))

    sizes = jnp.where(number % 4 == 0, named(packed, number // 4), named(common, number - number // 4 - 1))
    mixed = jax.random.permutation(jax.random.fold_in(own, 3), number_of)
    donor, taker = mixed[0:number_of // 2 * 2:2], mixed[1:number_of // 2 * 2:2]
    margin = jnp.minimum(sizes[donor] - 1, limit - sizes[taker]) // 2
    margin = jnp.where((donor == ranking[0]) | (taker == ranking[0]) | (sizes[taker] == 0), 0, jnp.maximum(margin, 0))
    moved = jax.random.randint(jax.random.fold_in(own, 4), (number_of // 2,), 0, 1 << 20) % (margin + 1)
    sizes = sizes.at[donor].add(-moved).at[taker].add(moved)
    members = jnp.searchsorted(jnp.cumsum(sizes), jnp.arange(rows * top), side="right").astype(jnp.int32)
    table = members.reshape(top, rows).T
    table = table[jax.random.permutation(jax.random.fold_in(own, 1), rows)]
    rotation = jax.random.randint(jax.random.fold_in(own, 2), (rows, 1), 0, top)
    return jnp.take_along_axis(table, (jnp.arange(top)[None, :] + rotation) % top, axis=1)


def shares(count, total, bound, slope, full):
    weights = [(1 << 20) // math.isqrt(standing ** slope) + 1 for standing in range(1, count + 1)]
    largest = bound if full else min(bound, max(-(-total // count), total * weights[0] // sum(weights)))
    least = 1 if total - largest >= count - 1 else 0
    counts, spare = [largest] + [least] * (count - 1), total - largest - least * (count - 1)
    while spare > 0:
        free = [i for i in range(1, count) if counts[i] < largest] or [i for i in range(1, count) if counts[i] < bound]
        mass, remaining = sum([weights[i] for i in free]), spare
        for i in free:
            more = min(bound - counts[i], max(1, remaining * weights[i] // mass), spare)
            counts[i] = counts[i] + more
            spare = spare - more
    return np.array(counts)


def setup_inputs(seed: int = 0) -> dict:
    splits = jax.random.split(jax.random.key(seed), 5)
    keys = place_ends(jax.random.randint(splits[0], (EXAMPLES,), 0, BINS * BIN_WIDTH), jax.random.fold_in(splits[0], 1), 0, (BINS * BIN_WIDTH) - 1).astype(jnp.int32)
    cut = jax.random.randint(splits[1], (1,), BINS // 16, BINS // 4).astype(jnp.int32)
    owner_keys = jax.random.split(jax.random.fold_in(splits[2], 1), EXAMPLES // EX_DEV)
    owner_turns = jax.random.permutation(jax.random.fold_in(splits[2], 3), EXAMPLES // EX_DEV)
    owner = jax.vmap(lambda own, number: deal_out(jax.random.fold_in(splits[2], 2), own, number, EX_DEV, N_DP, 1, MOST, 2))(owner_keys, owner_turns).reshape((EXAMPLES, 1))
    tokens = place_ends(ranked_wide(splits[3], (EXAMPLES, SEQ), VOCAB, 2), jax.random.fold_in(splits[3], 3), 0, VOCAB - 1).astype(jnp.int32)
    return {"keys": keys, "cut": cut, "owner": owner, "tokens": tokens}


def reference(keys, cut, owner, tokens):
    bins_of = keys // BIN_WIDTH
    hist = jnp.zeros((BINS,), jnp.float32).at[bins_of].add(1.0)
    kept = bins_of >= cut[0]
    dest = owner[:, 0]
    onehot = ((dest[:, None] == jnp.arange(N_DP, dtype=jnp.int32)[None, :]) & kept[:, None]).astype(jnp.int32)
    running = jnp.cumsum(onehot, axis=0) - onehot
    rank = jnp.sum(running * onehot, axis=1)
    device = dest * N_GROUP + rank % N_GROUP
    slot = rank // N_GROUP
    count = N_DP * N_GROUP * RECV
    target = jnp.where(kept, device * RECV + slot, count).astype(jnp.int32)
    suffix = jnp.cumsum(hist[::-1])[::-1]
    total = jnp.maximum(suffix[cut[0]], 1.0)
    weight = suffix[bins_of] / total
    packed_rows = jnp.zeros((count, SEQ), jnp.int32).at[target].set(tokens, mode="drop")
    packed_weights = jnp.zeros((count,), jnp.float32).at[target].set(weight, mode="drop")
    return hist.astype(jnp.int32), packed_rows, packed_weights
```

```python
import functools

import jax
import jax.numpy as jnp
from jax import lax
from jax.experimental import pallas as pl
from jax.experimental.pallas import tpu as pltpu
from jax.sharding import PartitionSpec as P

BINS = 4096
BIN_WIDTH = 262144
LANES = 128
MESH = pl.DeviceIdType.MESH


def peer(me, i, n):
    return lax.rem(me + 1 + lax.rem(i + n // 2 - 1, n - 1), n)


def place(d, n_member):
    return (lax.div(d, n_member), lax.rem(d, n_member))


def greet(me, n, n_member):
    barrier = pltpu.get_barrier_semaphore()

    def signal(i, c):
        pl.semaphore_signal(
            barrier, inc=1, device_id=place(peer(me, i, n), n_member), device_id_type=MESH
        )
        return c

    lax.fori_loop(0, n - 1, signal, 0)
    pl.semaphore_wait(barrier, n - 1)


def meta_kernel(n, n_member, mine, every, local_sem, send_sem, recv_sem):
    me = lax.axis_index("dp") * n_member + lax.axis_index("group")
    own = pltpu.make_async_copy(mine, every.at[me], local_sem)
    own.start()
    greet(me, n, n_member)

    def copy_to(d, sem):
        return pltpu.make_async_remote_copy(
            src_ref=mine,
            dst_ref=every.at[me],
            send_sem=send_sem.at[d],
            recv_sem=recv_sem.at[me],
            device_id=place(d, n_member),
            device_id_type=MESH,
        )

    def start(i, c):
        d = peer(me, i, n)
        copy_to(d, d).start()
        return c

    def finish(i, c):
        d = peer(me, i, n)
        copy = pltpu.make_async_remote_copy(
            src_ref=mine,
            dst_ref=every.at[d],
            send_sem=send_sem.at[d],
            recv_sem=recv_sem.at[d],
            device_id=place(d, n_member),
            device_id_type=MESH,
        )
        copy.wait_send()
        copy.wait_recv()
        return c

    lax.fori_loop(0, n - 1, start, 0)
    own.wait()
    lax.fori_loop(0, n - 1, finish, 0)


def rows_kernel(
    n, n_member, slots, pieces,
    index, tokens, key_send, keys_all,
    got, got_keys, hist,
    held, send, load_sem, own_sem, send_sem, recv_sem, ksend_sem, krecv_sem,
):
    me = lax.axis_index("dp") * n_member + lax.axis_index("group")
    loads = [
        pltpu.make_async_copy(
            tokens.at[:, pl.ds(p * LANES, LANES)], held.at[:, p, :], load_sem.at[p]
        )
        for p in range(pieces)
    ]
    for load in loads:
        load.start()
    greet(me, n, n_member)
    for load in loads:
        load.wait()

    def block(d):
        return pl.ds(d * slots, slots)

    def gather(d):
        for j in range(slots):
            send[d * slots + j] = held[index[d * slots + j]]

    def copies(d, at):
        rows = pltpu.make_async_remote_copy(
            src_ref=send.at[block(d)],
            dst_ref=got.at[block(at)],
            send_sem=send_sem.at[d],
            recv_sem=recv_sem.at[at],
            device_id=place(d, n_member),
            device_id_type=MESH,
        )
        keys = pltpu.make_async_remote_copy(
            src_ref=key_send.at[d],
            dst_ref=got_keys.at[at],
            send_sem=ksend_sem.at[d],
            recv_sem=krecv_sem.at[at],
            device_id=place(d, n_member),
            device_id_type=MESH,
        )
        return rows, keys

    gather(peer(me, 0, n))

    def start(i, c):
        gather(peer(me, i + 1, n))
        for copy in copies(peer(me, i, n), me):
            copy.start()
        return c

    lax.fori_loop(0, n - 2, start, 0)
    gather(me)
    for copy in copies(peer(me, n - 2, n), me):
        copy.start()
    own = pltpu.make_async_copy(send.at[block(me)], got.at[block(me)], own_sem.at[0])
    own_keys = pltpu.make_async_copy(key_send.at[me], got_keys.at[me], own_sem.at[1])
    own.start()
    own_keys.start()

    hist[...] = jnp.zeros_like(hist)
    hi_of = lax.broadcasted_iota(jnp.int32, (BINS // LANES, LANES), 0)
    lo_of = lax.broadcasted_iota(jnp.int32, (LANES, LANES), 0)

    def count(r, c):
        bins = keys_all[pl.ds(r, 1), :] // BIN_WIDTH
        hi = jnp.where(hi_of == bins // LANES, 1.0, 0.0).astype(jnp.bfloat16)
        lo = jnp.where(lo_of == bins % LANES, 1.0, 0.0).astype(jnp.bfloat16)
        hist[...] += lax.dot_general(
            hi, lo, (((1,), (1,)), ((), ())), preferred_element_type=jnp.float32
        )
        return c

    lax.fori_loop(0, keys_all.shape[0], count, 0)

    own.wait()
    own_keys.wait()

    def finish(i, c):
        d = peer(me, i, n)
        for copy in copies(d, d):
            copy.wait_send()
            copy.wait_recv()
        return c

    lax.fori_loop(0, n - 1, finish, 0)


def pack_kernel(pieces, chunk, index, got, out, held, made, load_sem, out_sem):
    rows = got.shape[0]
    load = pltpu.make_async_copy(got, held.at[pl.ds(0, rows)], load_sem)
    load.start()
    held[rows] = jnp.zeros(held.shape[1:], jnp.int32)
    load.wait()

    def stores(k):
        return [
            pltpu.make_async_copy(
                made.at[pl.ds(k * chunk, chunk), p, :],
                out.at[pl.ds(k * chunk, chunk), pl.ds(p * LANES, LANES)],
                out_sem.at[k, p],
            )
            for p in range(pieces)
        ]

    def fill(k):
        def some(g, c):
            for j in range(8):
                s = k * chunk + g * 8 + j
                made[s] = held[index[s]]
            return c

        lax.fori_loop(0, chunk // 8, some, 0)

    def step(k, c):
        fill(k)
        for copy in stores(k):
            copy.start()
        return c

    def finish(k, c):
        for copy in stores(k):
            copy.wait()
        return c

    lax.fori_loop(0, rows // chunk, step, 0)
    lax.fori_loop(0, rows // chunk, finish, 0)


def body(n_owner, n_member, keys, cut, owner, tokens):
    examples, width = tokens.shape
    n = n_owner * n_member
    slots = 2 * examples // n
    capacity = 2 * examples
    pieces = width // LANES
    per = examples // LANES
    me_dp, me_group = lax.axis_index("dp"), lax.axis_index("group")
    me = me_dp * n_member + me_group
    vmem = pl.BlockSpec(memory_space=pltpu.VMEM)
    smem = pl.BlockSpec(memory_space=pltpu.SMEM)
    hbm = pl.BlockSpec(memory_space=pl.ANY)
    dest = owner[:, 0]

    mine = jnp.concatenate([keys.reshape(per, LANES), dest.reshape(per, LANES)], axis=0)
    every = pl.pallas_call(
        functools.partial(meta_kernel, n, n_member),
        out_shape=jax.ShapeDtypeStruct((n, 2 * per, LANES), jnp.int32),
        in_specs=[vmem],
        out_specs=vmem,
        scratch_shapes=[
            pltpu.SemaphoreType.DMA,
            pltpu.SemaphoreType.DMA((n,)),
            pltpu.SemaphoreType.DMA((n,)),
        ],
        compiler_params=pltpu.CompilerParams(collective_id=0, has_side_effects=True),
    )(mine)
    keys_all = every[:, :per].reshape(n * per, LANES)
    owner_all = every[:, per:].reshape(n, examples)
    kept_all = keys_all.reshape(n, examples) // BIN_WIDTH >= cut[0]
    code_all = jnp.where(kept_all, owner_all, -1)
    table = jnp.sum(
        code_all[:, None, :] == jnp.arange(n_owner, dtype=jnp.int32)[None, :, None],
        axis=2, dtype=jnp.int32,
    )
    source = jnp.arange(n, dtype=jnp.int32)
    before = jnp.sum(jnp.where((source < me)[:, None], table, 0), axis=0)

    code = jnp.where(keys // BIN_WIDTH >= cut[0], dest, -1)
    e = jnp.arange(examples, dtype=jnp.int32)
    local_rank = jnp.sum(
        (code[:, None] == code[None, :]) & (e[None, :] < e[:, None]), axis=1, dtype=jnp.int32
    )
    spot = jnp.where(code >= 0, code * capacity + local_rank, -1)
    want = (
        jnp.arange(n_owner, dtype=jnp.int32)[:, None, None] * capacity
        + ((jnp.arange(n_member, dtype=jnp.int32)[None, :] - before[:, None]) % n_member)[:, :, None]
        + jnp.arange(slots, dtype=jnp.int32)[None, None, :] * n_member
    ).reshape(-1)
    match = want[:, None] == spot[None, :]
    index = jnp.sum(jnp.where(match, e[None, :], 0), axis=1)
    key_send = jnp.sum(jnp.where(match, keys[None, :], 0), axis=1)
    key_send = jnp.pad(key_send.reshape(n, 1, slots), ((0, 0), (0, 0), (0, LANES - slots)))

    got, got_keys, hist = pl.pallas_call(
        functools.partial(rows_kernel, n, n_member, slots, pieces),
        out_shape=(
            jax.ShapeDtypeStruct((capacity, pieces, LANES), jnp.int32),
            jax.ShapeDtypeStruct((n, 1, LANES), jnp.int32),
            jax.ShapeDtypeStruct((BINS // LANES, LANES), jnp.float32),
        ),
        in_specs=[smem, hbm, vmem, vmem],
        out_specs=(hbm, vmem, vmem),
        scratch_shapes=[
            pltpu.VMEM((examples, pieces, LANES), jnp.int32),
            pltpu.VMEM((capacity, pieces, LANES), jnp.int32),
            pltpu.SemaphoreType.DMA((pieces,)),
            pltpu.SemaphoreType.DMA((2,)),
            pltpu.SemaphoreType.DMA((n,)),
            pltpu.SemaphoreType.DMA((n,)),
            pltpu.SemaphoreType.DMA((n,)),
            pltpu.SemaphoreType.DMA((n,)),
        ],
        compiler_params=pltpu.CompilerParams(
            collective_id=1, has_side_effects=True, vmem_limit_bytes=60 * 1024 * 1024
        ),
    )(index, tokens, key_send, keys_all)
    hist = hist.reshape(BINS)

    arrived = jnp.sum(
        jnp.where(jnp.arange(n_owner, dtype=jnp.int32)[None, :] == me_dp, table, 0), axis=1
    )
    through = jnp.sum(jnp.where(source[None, :] <= source[:, None], arrived[None, :], 0), axis=1)
    rank = jnp.arange(capacity, dtype=jnp.int32) * n_member + me_group
    past = through[None, :] <= rank[:, None]
    origin = jnp.sum(past, axis=1, dtype=jnp.int32)
    start = jnp.sum(jnp.where(past, arrived[None, :], 0), axis=1)
    valid = origin < n
    pick = jnp.where(valid, origin * slots + (rank - start) // n_member, capacity)

    packed_rows = pl.pallas_call(
        functools.partial(pack_kernel, pieces, LANES),
        out_shape=jax.ShapeDtypeStruct((capacity, width), jnp.int32),
        in_specs=[smem, hbm],
        out_specs=hbm,
        scratch_shapes=[
            pltpu.VMEM((capacity + 1, pieces, LANES), jnp.int32),
            pltpu.VMEM((capacity, pieces, LANES), jnp.int32),
            pltpu.SemaphoreType.DMA,
            pltpu.SemaphoreType.DMA((capacity // LANES, pieces)),
        ],
        compiler_params=pltpu.CompilerParams(vmem_limit_bytes=60 * 1024 * 1024),
    )(pick, got)

    b = jnp.arange(BINS, dtype=jnp.int32)
    total = jnp.maximum(jnp.sum(jnp.where(b >= cut[0], hist, 0.0)), 1.0)
    bins = got_keys[:, 0, :slots].reshape(-1) // BIN_WIDTH
    above = jnp.sum(jnp.where(b[None, :] >= bins[:, None], hist[None, :], 0.0), axis=1)
    place_of = jnp.arange(capacity, dtype=jnp.int32)
    value = jnp.sum(jnp.where(pick[:, None] == place_of[None, :], above[None, :], 0.0), axis=1)
    packed_weights = value / total
    return (hist.astype(jnp.int32), packed_rows, packed_weights)


def solution(mesh):
    placed = (P(("dp", "group")), P(), P(("dp", "group"), None), P(("dp", "group"), None))
    return jax.shard_map(
        functools.partial(body, mesh.shape["dp"], mesh.shape["group"]),
        mesh=mesh,
        in_specs=placed,
        out_specs=(P(), P(("dp", "group"), None), P(("dp", "group"))),
        check_vma=False,
    )
```

```python
import functools
import itertools
import math

import jax
import jax.numpy as jnp
import numpy as np
from jax import lax
from jax.experimental import pallas as pl
from jax.experimental.pallas import tpu as pltpu
from jax.sharding import PartitionSpec as P

BINS = 4096
BIN_WIDTH = 262144
LANES = 128
MESH = pl.DeviceIdType.MESH


def peer(me, i, n):
    return lax.rem(me + 1 + lax.rem(i + n // 2 - 1, n - 1), n)


def place(d, n_member):
    return (lax.div(d, n_member), lax.rem(d, n_member))


def greet(me, n, n_member):
    barrier = pltpu.get_barrier_semaphore()

    def signal(i, c):
        pl.semaphore_signal(
            barrier, inc=1, device_id=place(peer(me, i, n), n_member), device_id_type=MESH
        )
        return c

    lax.fori_loop(0, n - 1, signal, 0)
    pl.semaphore_wait(barrier, n - 1)


def meta_kernel(n, n_member, mine, every, local_sem, send_sem, recv_sem):
    me = lax.axis_index("dp") * n_member + lax.axis_index("group")
    own = pltpu.make_async_copy(mine, every.at[me], local_sem)
    own.start()
    greet(me, n, n_member)

    def copy_to(d, sem):
        return pltpu.make_async_remote_copy(
            src_ref=mine,
            dst_ref=every.at[me],
            send_sem=send_sem.at[d],
            recv_sem=recv_sem.at[me],
            device_id=place(d, n_member),
            device_id_type=MESH,
        )

    def start(i, c):
        d = peer(me, i, n)
        copy_to(d, d).start()
        return c

    def finish(i, c):
        d = peer(me, i, n)
        copy = pltpu.make_async_remote_copy(
            src_ref=mine,
            dst_ref=every.at[d],
            send_sem=send_sem.at[d],
            recv_sem=recv_sem.at[d],
            device_id=place(d, n_member),
            device_id_type=MESH,
        )
        copy.wait_send()
        copy.wait_recv()
        return c

    lax.fori_loop(0, n - 1, start, 0)
    own.wait()
    lax.fori_loop(0, n - 1, finish, 0)


def rows_kernel(
    n, n_member, slots, base, wide, pieces,
    index, tokens, key_send, keys_all,
    got, got_keys, hist,
    held, send, load_sem, own_sem, send_sem, recv_sem, ksend_sem, krecv_sem, more_sem, mrecv_sem,
):
    me = lax.axis_index("dp") * n_member + lax.axis_index("group")
    loads = [
        pltpu.make_async_copy(
            tokens.at[:, pl.ds(p * LANES, LANES)], held.at[:, p, :], load_sem.at[p]
        )
        for p in range(pieces)
    ]
    for load in loads:
        load.start()
    greet(me, n, n_member)
    for load in loads:
        load.wait()

    def block(d):
        return pl.ds(d * slots, slots)

    def is_wide(d):
        at = lax.div(d, n_member)
        found = at == wide[0]
        for o in wide[1:]:
            found = jnp.logical_or(found, at == o)
        return found

    def fill(d, first, last):
        group = math.gcd(math.gcd(first, last), 8)

        def some(g, c):
            for j in range(group):
                at = d * slots + first + g * group + j
                send[at] = held[index[at]]
            return c

        lax.fori_loop(0, (last - first) // group, some, 0)

    def gather(d):
        fill(d, 0, base)
        if base < slots:
            pl.when(is_wide(d))(functools.partial(fill, d, base, slots))

    def row_copy(d, at, first, size, out_sem, in_sem):
        return pltpu.make_async_remote_copy(
            src_ref=send.at[pl.ds(d * slots + first, size)],
            dst_ref=got.at[pl.ds(at * slots + first, size)],
            send_sem=out_sem.at[d],
            recv_sem=in_sem.at[at],
            device_id=place(d, n_member),
            device_id_type=MESH,
        )

    def more(d, at):
        return row_copy(d, at, base, slots - base, more_sem, mrecv_sem)

    def copies(d, at):
        rows = row_copy(d, at, 0, base, send_sem, recv_sem)
        keys = pltpu.make_async_remote_copy(
            src_ref=key_send.at[d],
            dst_ref=got_keys.at[at],
            send_sem=ksend_sem.at[d],
            recv_sem=krecv_sem.at[at],
            device_id=place(d, n_member),
            device_id_type=MESH,
        )
        return rows, keys

    def send_to(d):
        for copy in copies(d, me):
            copy.start()
        if base < slots:
            pl.when(is_wide(d))(lambda: more(d, me).start())

    gather(peer(me, 0, n))

    def start(i, c):
        gather(peer(me, i + 1, n))
        send_to(peer(me, i, n))
        return c

    lax.fori_loop(0, n - 2, start, 0)
    fill(me, 0, slots)
    send_to(peer(me, n - 2, n))
    own = pltpu.make_async_copy(send.at[block(me)], got.at[block(me)], own_sem.at[0])
    own_keys = pltpu.make_async_copy(key_send.at[me], got_keys.at[me], own_sem.at[1])
    own.start()
    own_keys.start()

    hist[...] = jnp.zeros_like(hist)
    hi_of = lax.broadcasted_iota(jnp.int32, (BINS // LANES, LANES), 0)
    lo_of = lax.broadcasted_iota(jnp.int32, (LANES, LANES), 0)

    def count(r, c):
        bins = keys_all[pl.ds(r, 1), :] // BIN_WIDTH
        hi = jnp.where(hi_of == bins // LANES, 1.0, 0.0).astype(jnp.bfloat16)
        lo = jnp.where(lo_of == bins % LANES, 1.0, 0.0).astype(jnp.bfloat16)
        hist[...] += lax.dot_general(
            hi, lo, (((1,), (1,)), ((), ())), preferred_element_type=jnp.float32
        )
        return c

    lax.fori_loop(0, keys_all.shape[0], count, 0)

    own.wait()
    own_keys.wait()

    def finish(i, c):
        d = peer(me, i, n)
        for copy in copies(d, d):
            copy.wait_send()
            copy.wait_recv()
        if base < slots:
            pl.when(is_wide(d))(lambda: more(d, d).wait_send())
            pl.when(is_wide(me))(lambda: more(d, d).wait_recv())
        return c

    lax.fori_loop(0, n - 1, finish, 0)


def pack_kernel(pieces, chunk, index, got, out, held, made, load_sem, out_sem):
    rows = got.shape[0]
    load = pltpu.make_async_copy(got, held.at[pl.ds(0, rows)], load_sem)
    load.start()
    held[rows] = jnp.zeros(held.shape[1:], jnp.int32)
    load.wait()

    def stores(k):
        return [
            pltpu.make_async_copy(
                made.at[pl.ds(k * chunk, chunk), p, :],
                out.at[pl.ds(k * chunk, chunk), pl.ds(p * LANES, LANES)],
                out_sem.at[k, p],
            )
            for p in range(pieces)
        ]

    def fill(k):
        def some(g, c):
            for j in range(8):
                s = k * chunk + g * 8 + j
                made[s] = held[index[s]]
            return c

        lax.fori_loop(0, chunk // 8, some, 0)

    def step(k, c):
        fill(k)
        for copy in stores(k):
            copy.start()
        return c

    def finish(k, c):
        for copy in stores(k):
            copy.wait()
        return c

    lax.fori_loop(0, rows // chunk, step, 0)
    lax.fori_loop(0, rows // chunk, finish, 0)


def body(n_owner, n_member, keys, cut, owner, tokens):
    examples, width = tokens.shape
    n = n_owner * n_member
    slots = 2 * examples // n
    capacity = 2 * examples
    pieces = width // LANES
    per = examples // LANES
    me_dp, me_group = lax.axis_index("dp"), lax.axis_index("group")
    me = me_dp * n_member + me_group
    vmem = pl.BlockSpec(memory_space=pltpu.VMEM)
    smem = pl.BlockSpec(memory_space=pltpu.SMEM)
    hbm = pl.BlockSpec(memory_space=pl.ANY)
    dest = owner[:, 0]

    mine = jnp.concatenate([keys.reshape(per, LANES), dest.reshape(per, LANES)], axis=0)
    every = pl.pallas_call(
        functools.partial(meta_kernel, n, n_member),
        out_shape=jax.ShapeDtypeStruct((n, 2 * per, LANES), jnp.int32),
        in_specs=[vmem],
        out_specs=vmem,
        scratch_shapes=[
            pltpu.SemaphoreType.DMA,
            pltpu.SemaphoreType.DMA((n,)),
            pltpu.SemaphoreType.DMA((n,)),
        ],
        compiler_params=pltpu.CompilerParams(collective_id=0, has_side_effects=True),
    )(mine)
    keys_all = every[:, :per].reshape(n * per, LANES)
    owner_all = every[:, per:].reshape(n, examples)
    kept_all = keys_all.reshape(n, examples) // BIN_WIDTH >= cut[0]
    code_all = jnp.where(kept_all, owner_all, -1)
    table = jnp.sum(
        code_all[:, None, :] == jnp.arange(n_owner, dtype=jnp.int32)[None, :, None],
        axis=2, dtype=jnp.int32,
    )
    source = jnp.arange(n, dtype=jnp.int32)
    before = jnp.sum(jnp.where((source < me)[:, None], table, 0), axis=0)

    code = jnp.where(keys // BIN_WIDTH >= cut[0], dest, -1)
    e = jnp.arange(examples, dtype=jnp.int32)
    local_rank = jnp.sum(
        (code[:, None] == code[None, :]) & (e[None, :] < e[:, None]), axis=1, dtype=jnp.int32
    )
    spot = jnp.where(code >= 0, code * capacity + local_rank, -1)
    want = (
        jnp.arange(n_owner, dtype=jnp.int32)[:, None, None] * capacity
        + ((jnp.arange(n_member, dtype=jnp.int32)[None, :] - before[:, None]) % n_member)[:, :, None]
        + jnp.arange(slots, dtype=jnp.int32)[None, None, :] * n_member
    ).reshape(-1)
    match = want[:, None] == spot[None, :]
    index = jnp.sum(jnp.where(match, e[None, :], 0), axis=1)
    key_send = jnp.sum(jnp.where(match, keys[None, :], 0), axis=1)
    key_send = jnp.pad(key_send.reshape(n, 1, slots), ((0, 0), (0, 0), (0, LANES - slots)))

    def exchange(number, base, wide):
        return pl.pallas_call(
            functools.partial(rows_kernel, n, n_member, slots, base, wide, pieces),
            out_shape=(
                jax.ShapeDtypeStruct((capacity, pieces, LANES), jnp.int32),
                jax.ShapeDtypeStruct((n, 1, LANES), jnp.int32),
                jax.ShapeDtypeStruct((BINS // LANES, LANES), jnp.float32),
            ),
            in_specs=[smem, hbm, vmem, vmem],
            out_specs=(hbm, vmem, vmem),
            scratch_shapes=[
                pltpu.VMEM((examples, pieces, LANES), jnp.int32),
                pltpu.VMEM((capacity, pieces, LANES), jnp.int32),
                pltpu.SemaphoreType.DMA((pieces,)),
                pltpu.SemaphoreType.DMA((2,)),
            ]
            + [pltpu.SemaphoreType.DMA((n,))] * 6,
            compiler_params=pltpu.CompilerParams(
                collective_id=1 + number, has_side_effects=True,
                vmem_limit_bytes=60 * 1024 * 1024,
            ),
        )

    base = slots * 3 // 4
    pairs = list(itertools.combinations(range(n_owner), 2))
    pairs = pairs if len(pairs) <= 32 else []
    needs = jnp.max(table, axis=0) > base * n_member
    choice = jnp.int32(0)
    if pairs:
        member_of = np.zeros((len(pairs), n_owner), bool)
        for p, pair in enumerate(pairs):
            member_of[p, list(pair)] = True
        fits = jnp.all(jnp.logical_or(member_of, ~needs[None, :]), axis=1)
        choice = jnp.max(jnp.where(fits, jnp.arange(1, len(pairs) + 1, dtype=jnp.int32), 0))
    calls = [exchange(0, slots, ())]
    for number, pair in enumerate(pairs, 1):
        calls.append(exchange(number, base, pair))
    choice, index, key_send, keys_all = lax.optimization_barrier(
        (choice, index, key_send, keys_all)
    )
    got, got_keys, hist = lax.switch(choice, calls, index, tokens, key_send, keys_all)
    hist = hist.reshape(BINS)

    arrived = jnp.sum(
        jnp.where(jnp.arange(n_owner, dtype=jnp.int32)[None, :] == me_dp, table, 0), axis=1
    )
    through = jnp.sum(jnp.where(source[None, :] <= source[:, None], arrived[None, :], 0), axis=1)
    rank = jnp.arange(capacity, dtype=jnp.int32) * n_member + me_group
    past = through[None, :] <= rank[:, None]
    origin = jnp.sum(past, axis=1, dtype=jnp.int32)
    start = jnp.sum(jnp.where(past, arrived[None, :], 0), axis=1)
    valid = origin < n
    pick = jnp.where(valid, origin * slots + (rank - start) // n_member, capacity)

    packed_rows = pl.pallas_call(
        functools.partial(pack_kernel, pieces, LANES),
        out_shape=jax.ShapeDtypeStruct((capacity, width), jnp.int32),
        in_specs=[smem, hbm],
        out_specs=hbm,
        scratch_shapes=[
            pltpu.VMEM((capacity + 1, pieces, LANES), jnp.int32),
            pltpu.VMEM((capacity, pieces, LANES), jnp.int32),
            pltpu.SemaphoreType.DMA,
            pltpu.SemaphoreType.DMA((capacity // LANES, pieces)),
        ],
        compiler_params=pltpu.CompilerParams(vmem_limit_bytes=60 * 1024 * 1024),
    )(pick, got)

    b = jnp.arange(BINS, dtype=jnp.int32)
    total = jnp.maximum(jnp.sum(jnp.where(b >= cut[0], hist, 0.0)), 1.0)
    bins = got_keys[:, 0, :slots].reshape(-1) // BIN_WIDTH
    above = jnp.sum(jnp.where(b[None, :] >= bins[:, None], hist[None, :], 0.0), axis=1)
    place_of = jnp.arange(capacity, dtype=jnp.int32)
    value = jnp.sum(jnp.where(pick[:, None] == place_of[None, :], above[None, :], 0.0), axis=1)
    packed_weights = value / total
    return (hist.astype(jnp.int32), packed_rows, packed_weights)


def solution(mesh):
    placed = (P(("dp", "group")), P(), P(("dp", "group"), None), P(("dp", "group"), None))
    return jax.shard_map(
        functools.partial(body, mesh.shape["dp"], mesh.shape["group"]),
        mesh=mesh,
        in_specs=placed,
        out_specs=(P(), P(("dp", "group"), None), P(("dp", "group"))),
        check_vma=False,
    )
```

```python
import functools
import itertools
import math

import jax
import jax.numpy as jnp
import numpy as np
from jax import lax
from jax.experimental import pallas as pl
from jax.experimental.pallas import tpu as pltpu
from jax.sharding import PartitionSpec as P

BINS = 4096
BIN_WIDTH = 262144
LANES = 128
MESH = pl.DeviceIdType.MESH


def peer(me, i, n):
    return lax.rem(me + 1 + lax.rem(i + n // 2 - 1, n - 1), n)


def place(d, n_member):
    return (lax.div(d, n_member), lax.rem(d, n_member))


def greet(me, n, n_member):
    barrier = pltpu.get_barrier_semaphore()

    def signal(i, c):
        pl.semaphore_signal(
            barrier, inc=1, device_id=place(peer(me, i, n), n_member), device_id_type=MESH
        )
        return c

    lax.fori_loop(0, n - 1, signal, 0)
    pl.semaphore_wait(barrier, n - 1)


def meta_kernel(n, n_member, mine, every, local_sem, send_sem, recv_sem):
    me = lax.axis_index("dp") * n_member + lax.axis_index("group")
    own = pltpu.make_async_copy(mine, every.at[me], local_sem)
    own.start()
    greet(me, n, n_member)

    def copy_to(d, sem):
        return pltpu.make_async_remote_copy(
            src_ref=mine,
            dst_ref=every.at[me],
            send_sem=send_sem.at[d],
            recv_sem=recv_sem.at[me],
            device_id=place(d, n_member),
            device_id_type=MESH,
        )

    def start(i, c):
        d = peer(me, i, n)
        copy_to(d, d).start()
        return c

    def finish(i, c):
        d = peer(me, i, n)
        copy = pltpu.make_async_remote_copy(
            src_ref=mine,
            dst_ref=every.at[d],
            send_sem=send_sem.at[d],
            recv_sem=recv_sem.at[d],
            device_id=place(d, n_member),
            device_id_type=MESH,
        )
        copy.wait_send()
        copy.wait_recv()
        return c

    lax.fori_loop(0, n - 1, start, 0)
    own.wait()
    lax.fori_loop(0, n - 1, finish, 0)


def rows_kernel(
    n, n_member, slots, base, wide, pieces,
    index, tokens, key_send, keys_all,
    got, got_keys, hist,
    held, send, load_sem, own_sem, send_sem, recv_sem, ksend_sem, krecv_sem, more_sem, mrecv_sem,
):
    me = lax.axis_index("dp") * n_member + lax.axis_index("group")
    loads = [
        pltpu.make_async_copy(
            tokens.at[:, pl.ds(p * LANES, LANES)], held.at[:, p, :], load_sem.at[p]
        )
        for p in range(pieces)
    ]
    for load in loads:
        load.start()
    greet(me, n, n_member)
    for load in loads:
        load.wait()

    def block(d):
        return pl.ds(d * slots, slots)

    def is_wide(d):
        at = lax.div(d, n_member)
        found = at == wide[0]
        for o in wide[1:]:
            found = jnp.logical_or(found, at == o)
        return found

    def fill(d, first, last):
        group = math.gcd(math.gcd(first, last), 8)

        def some(g, c):
            for j in range(group):
                at = d * slots + first + g * group + j
                send[at] = held[index[at]]
            return c

        lax.fori_loop(0, (last - first) // group, some, 0)

    def gather(d):
        fill(d, 0, base)
        if base < slots:
            pl.when(is_wide(d))(functools.partial(fill, d, base, slots))

    def row_copy(d, at, first, size, out_sem, in_sem):
        return pltpu.make_async_remote_copy(
            src_ref=send.at[pl.ds(d * slots + first, size)],
            dst_ref=got.at[pl.ds(at * slots + first, size)],
            send_sem=out_sem.at[d],
            recv_sem=in_sem.at[at],
            device_id=place(d, n_member),
            device_id_type=MESH,
        )

    def more(d, at):
        return row_copy(d, at, base, slots - base, more_sem, mrecv_sem)

    def copies(d, at):
        rows = row_copy(d, at, 0, base, send_sem, recv_sem)
        keys = pltpu.make_async_remote_copy(
            src_ref=key_send.at[d],
            dst_ref=got_keys.at[at],
            send_sem=ksend_sem.at[d],
            recv_sem=krecv_sem.at[at],
            device_id=place(d, n_member),
            device_id_type=MESH,
        )
        return rows, keys

    def send_to(d):
        for copy in copies(d, me):
            copy.start()
        if base < slots:
            pl.when(is_wide(d))(lambda: more(d, me).start())

    gather(peer(me, 0, n))

    def start(i, c):
        gather(peer(me, i + 1, n))
        send_to(peer(me, i, n))
        return c

    lax.fori_loop(0, n - 2, start, 0)
    fill(me, 0, slots)
    send_to(peer(me, n - 2, n))
    own = pltpu.make_async_copy(send.at[block(me)], got.at[block(me)], own_sem.at[0])
    own_keys = pltpu.make_async_copy(key_send.at[me], got_keys.at[me], own_sem.at[1])
    own.start()
    own_keys.start()

    hist[...] = jnp.zeros_like(hist)
    hi_of = lax.broadcasted_iota(jnp.int32, (BINS // LANES, LANES), 0)
    lo_of = lax.broadcasted_iota(jnp.int32, (LANES, LANES), 0)

    def count(r, c):
        bins = keys_all[pl.ds(r, 1), :] // BIN_WIDTH
        hi = jnp.where(hi_of == bins // LANES, 1.0, 0.0).astype(jnp.bfloat16)
        lo = jnp.where(lo_of == bins % LANES, 1.0, 0.0).astype(jnp.bfloat16)
        hist[...] += lax.dot_general(
            hi, lo, (((1,), (1,)), ((), ())), preferred_element_type=jnp.float32
        )
        return c

    lax.fori_loop(0, keys_all.shape[0], count, 0)

    own.wait()
    own_keys.wait()

    def finish(i, c):
        d = peer(me, i, n)
        for copy in copies(d, d):
            copy.wait_send()
            copy.wait_recv()
        if base < slots:
            pl.when(is_wide(d))(lambda: more(d, d).wait_send())
            pl.when(is_wide(me))(lambda: more(d, d).wait_recv())
        return c

    lax.fori_loop(0, n - 1, finish, 0)


def pack_kernel(pieces, chunk, index, need, got, out, held, made, load_sem, out_sem):
    rows = got.shape[0]

    def load(q):
        part = pl.ds(q * chunk, chunk)
        return pltpu.make_async_copy(got.at[part], held.at[part], load_sem.at[q])

    def begin(q, c):
        load(q).start()
        return c

    def arrive(q, c):
        load(q).wait()
        return c

    lax.fori_loop(0, rows // chunk, begin, 0)
    held[rows] = jnp.zeros(held.shape[1:], jnp.int32)

    def stores(k):
        return [
            pltpu.make_async_copy(
                made.at[pl.ds(k * chunk, chunk), p, :],
                out.at[pl.ds(k * chunk, chunk), pl.ds(p * LANES, LANES)],
                out_sem.at[k, p],
            )
            for p in range(pieces)
        ]

    def fill(k):
        def some(g, c):
            for j in range(8):
                s = k * chunk + g * 8 + j
                made[s] = held[index[s]]
            return c

        lax.fori_loop(0, chunk // 8, some, 0)

    def step(k, ready):
        upto = jnp.maximum(ready, need[k])
        lax.fori_loop(ready, upto, arrive, 0)
        fill(k)
        for copy in stores(k):
            copy.start()
        return upto

    def finish(k, c):
        for copy in stores(k):
            copy.wait()
        return c

    ready = lax.fori_loop(0, rows // chunk, step, jnp.int32(0))
    lax.fori_loop(ready, rows // chunk, arrive, 0)
    lax.fori_loop(0, rows // chunk, finish, 0)


def body(n_owner, n_member, keys, cut, owner, tokens):
    examples, width = tokens.shape
    n = n_owner * n_member
    slots = 2 * examples // n
    capacity = 2 * examples
    pieces = width // LANES
    per = examples // LANES
    me_dp, me_group = lax.axis_index("dp"), lax.axis_index("group")
    me = me_dp * n_member + me_group
    vmem = pl.BlockSpec(memory_space=pltpu.VMEM)
    smem = pl.BlockSpec(memory_space=pltpu.SMEM)
    hbm = pl.BlockSpec(memory_space=pl.ANY)
    dest = owner[:, 0]

    mine = jnp.concatenate([keys.reshape(per, LANES), dest.reshape(per, LANES)], axis=0)
    every = pl.pallas_call(
        functools.partial(meta_kernel, n, n_member),
        out_shape=jax.ShapeDtypeStruct((n, 2 * per, LANES), jnp.int32),
        in_specs=[vmem],
        out_specs=vmem,
        scratch_shapes=[
            pltpu.SemaphoreType.DMA,
            pltpu.SemaphoreType.DMA((n,)),
            pltpu.SemaphoreType.DMA((n,)),
        ],
        compiler_params=pltpu.CompilerParams(collective_id=0, has_side_effects=True),
    )(mine)
    keys_all = every[:, :per].reshape(n * per, LANES)
    owner_all = every[:, per:].reshape(n, examples)
    kept_all = keys_all.reshape(n, examples) // BIN_WIDTH >= cut[0]
    code_all = jnp.where(kept_all, owner_all, -1)
    table = jnp.sum(
        code_all[:, None, :] == jnp.arange(n_owner, dtype=jnp.int32)[None, :, None],
        axis=2, dtype=jnp.int32,
    )
    source = jnp.arange(n, dtype=jnp.int32)
    before = jnp.sum(jnp.where((source < me)[:, None], table, 0), axis=0)

    code = jnp.where(keys // BIN_WIDTH >= cut[0], dest, -1)
    e = jnp.arange(examples, dtype=jnp.int32)
    local_rank = jnp.sum(
        (code[:, None] == code[None, :]) & (e[None, :] < e[:, None]), axis=1, dtype=jnp.int32
    )
    spot = jnp.where(code >= 0, code * capacity + local_rank, -1)
    want = (
        jnp.arange(n_owner, dtype=jnp.int32)[:, None, None] * capacity
        + ((jnp.arange(n_member, dtype=jnp.int32)[None, :] - before[:, None]) % n_member)[:, :, None]
        + jnp.arange(slots, dtype=jnp.int32)[None, None, :] * n_member
    ).reshape(-1)
    match = want[:, None] == spot[None, :]
    index = jnp.sum(jnp.where(match, e[None, :], 0), axis=1)
    key_send = jnp.sum(jnp.where(match, keys[None, :], 0), axis=1)
    key_send = jnp.pad(key_send.reshape(n, 1, slots), ((0, 0), (0, 0), (0, LANES - slots)))

    def exchange(number, base, wide):
        return pl.pallas_call(
            functools.partial(rows_kernel, n, n_member, slots, base, wide, pieces),
            out_shape=(
                jax.ShapeDtypeStruct((capacity, pieces, LANES), jnp.int32),
                jax.ShapeDtypeStruct((n, 1, LANES), jnp.int32),
                jax.ShapeDtypeStruct((BINS // LANES, LANES), jnp.float32),
            ),
            in_specs=[smem, hbm, vmem, vmem],
            out_specs=(hbm, vmem, vmem),
            scratch_shapes=[
                pltpu.VMEM((examples, pieces, LANES), jnp.int32),
                pltpu.VMEM((capacity, pieces, LANES), jnp.int32),
                pltpu.SemaphoreType.DMA((pieces,)),
                pltpu.SemaphoreType.DMA((2,)),
            ]
            + [pltpu.SemaphoreType.DMA((n,))] * 6,
            compiler_params=pltpu.CompilerParams(
                collective_id=1 + number, has_side_effects=True,
                vmem_limit_bytes=60 * 1024 * 1024,
            ),
        )

    base = slots * 3 // 4
    pairs = list(itertools.combinations(range(n_owner), 2))
    pairs = pairs if len(pairs) <= 32 else []
    needs = jnp.max(table, axis=0) > base * n_member
    choice = jnp.int32(0)
    if pairs:
        member_of = np.zeros((len(pairs), n_owner), bool)
        for p, pair in enumerate(pairs):
            member_of[p, list(pair)] = True
        fits = jnp.all(jnp.logical_or(member_of, ~needs[None, :]), axis=1)
        choice = jnp.max(jnp.where(fits, jnp.arange(1, len(pairs) + 1, dtype=jnp.int32), 0))
    calls = [exchange(0, slots, ())]
    for number, pair in enumerate(pairs, 1):
        calls.append(exchange(number, base, pair))
    choice, index, key_send, keys_all = lax.optimization_barrier(
        (choice, index, key_send, keys_all)
    )
    got, got_keys, hist = lax.switch(choice, calls, index, tokens, key_send, keys_all)
    hist = hist.reshape(BINS)

    arrived = jnp.sum(
        jnp.where(jnp.arange(n_owner, dtype=jnp.int32)[None, :] == me_dp, table, 0), axis=1
    )
    through = jnp.sum(jnp.where(source[None, :] <= source[:, None], arrived[None, :], 0), axis=1)
    rank = jnp.arange(capacity, dtype=jnp.int32) * n_member + me_group
    past = through[None, :] <= rank[:, None]
    origin = jnp.sum(past, axis=1, dtype=jnp.int32)
    start = jnp.sum(jnp.where(past, arrived[None, :], 0), axis=1)
    valid = origin < n
    pick = jnp.where(valid, origin * slots + (rank - start) // n_member, capacity)

    need = jnp.max(jnp.where(valid, pick // LANES + 1, 0).reshape(-1, LANES), axis=1)
    packed_rows = pl.pallas_call(
        functools.partial(pack_kernel, pieces, LANES),
        out_shape=jax.ShapeDtypeStruct((capacity, width), jnp.int32),
        in_specs=[smem, smem, hbm],
        out_specs=hbm,
        scratch_shapes=[
            pltpu.VMEM((capacity + 1, pieces, LANES), jnp.int32),
            pltpu.VMEM((capacity, pieces, LANES), jnp.int32),
            pltpu.SemaphoreType.DMA((capacity // LANES,)),
            pltpu.SemaphoreType.DMA((capacity // LANES, pieces)),
        ],
        compiler_params=pltpu.CompilerParams(vmem_limit_bytes=60 * 1024 * 1024),
    )(pick, need, got)

    b = jnp.arange(BINS, dtype=jnp.int32)
    total = jnp.maximum(jnp.sum(jnp.where(b >= cut[0], hist, 0.0)), 1.0)
    bins = got_keys[:, 0, :slots].reshape(-1) // BIN_WIDTH
    above = jnp.sum(jnp.where(b[None, :] >= bins[:, None], hist[None, :], 0.0), axis=1)
    place_of = jnp.arange(capacity, dtype=jnp.int32)
    value = jnp.sum(jnp.where(pick[:, None] == place_of[None, :], above[None, :], 0.0), axis=1)
    packed_weights = value / total
    return (hist.astype(jnp.int32), packed_rows, packed_weights)


def solution(mesh):
    placed = (P(("dp", "group")), P(), P(("dp", "group"), None), P(("dp", "group"), None))
    return jax.shard_map(
        functools.partial(body, mesh.shape["dp"], mesh.shape["group"]),
        mesh=mesh,
        in_specs=placed,
        out_specs=(P(), P(("dp", "group"), None), P(("dp", "group"))),
        check_vma=False,
    )
```
